32 devices in a mesh: row: 8 (over z, core), col: 4 (over y, x).
Axes of the slice: x: 2, y: 2, z: 4, core: 2. Of those that a mesh axis runs over, the one named last changes fastest.
Arguments:
- right_sides: float32 [4, 1024, 4096], P(None, 'row', 'col'), may hold values from -6 to 6
- low_left: bfloat16 [6, 4096, 128], P(None, 'col'), may hold values from -0.25 to 0.25
- low_right: bfloat16 [6, 4096, 128], P(None, 'col'), may hold values from -0.09375 to 0.09375
- up_left: bfloat16 [6, 4096, 128], P(None, 'col'), may hold values from -0.25 to 0.25
- up_right: bfloat16 [6, 4096, 128], P(None, 'col'), may hold values from -0.09375 to 0.09375
- low_ranks: int32 [6], replicated, may hold values from 1 to 4
- up_ranks: int32 [6], replicated, may hold values from 1 to 4
- inv_lower: bfloat16 [4, 4096, 4096], P(None, 'col', 'row'), may hold values from -0.09375 to 0.09375
- inv_upper: bfloat16 [4, 4096, 4096], P(None, 'col', 'row'), may hold values from -0.09375 to 0.09375
Outputs:
- solution: float32 [4, 1024, 4096], P(None, 'row', 'col')
The draws below stay inside these ranges and needn't reach their ends.
Inputs may be any that keep to these rules, and one draw needn't show every extreme that they name: `low_ranks`: factor columns beyond 32 times this value are padding with arbitrary values and must be masked out. `up_ranks`: factor columns beyond 32 times this value are padding with arbitrary values and must be masked out.
All inputs are finite; a program needn't handle non-finite values.
Results may differ from the reference program's by a relative error of at most 0.03.
Values may be sent and summed in bfloat16 or wider, within the bound.
A program may use at most 64 MiB of HBM per device.

```python
import jax
import jax.numpy as jnp
import numpy as np
from jax import lax

B = 4096
RBLK = 32
R = 128
NT = 4
NRHS = 1024
PAIRS = 6


def touch_ends(result, rng, low, top_value):
    longest = result.shape.index(max(result.shape))
    spots = []
    for shift in (0, 1):
        where = [jax.random.randint(jax.random.fold_in(rng, axis), (), 0, length) for axis, length in enumerate(result.shape)]
        where[longest] = (where[longest] + shift) % result.shape[longest]
        spots.append(tuple(where))
    return result.at[spots[0]].set(low).at[spots[1]].set(top_value)


def shard_levels(own_key, shape, cuts, low, largest):
    loudness = 1.0
    for axis_at, blocks in cuts:
        draws = jax.random.uniform(jax.random.fold_in(jax.random.fold_in(own_key, 6), axis_at), (blocks,), jnp.float32, low / len(cuts), largest / len(cuts))
        loudness = loudness * jnp.repeat(jnp.exp(draws), shape[axis_at] // blocks).reshape((-1,) + (1,) * (len(shape) - 1 - axis_at))
    return loudness


def gaussian(stream_key, extent, deviation, bound, shards=(), held_as=jnp.bfloat16):
    values = jax.random.normal(stream_key, extent, jnp.float32) * deviation
    if len(shards) > 0:
        values = shard_levels(stream_key, extent, shards, -0.22, 0.18) * values
    return jnp.clip(values, min=-bound, max=bound).astype(held_as)


def setup_inputs(seed: int = 0) -> dict:
    arg_keys = jax.random.split(jax.random.key(seed), 10)
    return {
        "right_sides": gaussian(arg_keys[0], (NT, NRHS, B), 1.0, 6.0, ((1, 8), (2, 4)), jnp.float32),
        "low_left": gaussian(arg_keys[1], (PAIRS, B, R), (4 * R) ** -0.5, 0.25, ((1, 4),)),
        "low_right": gaussian(arg_keys[2], (PAIRS, B, R), B ** -0.5, 0.09375, ((1, 4),)),
        "up_left": gaussian(arg_keys[3], (PAIRS, B, R), (4 * R) ** -0.5, 0.25, ((1, 4),)),
        "up_right": gaussian(arg_keys[4], (PAIRS, B, R), B ** -0.5, 0.09375, ((1, 4),)),
        "low_ranks": touch_ends(jax.random.randint(arg_keys[5], (PAIRS,), 1, 5), jax.random.fold_in(arg_keys[5], 1), 1, 4).astype(jnp.int32),
        "up_ranks": touch_ends(jax.random.randint(arg_keys[6], (PAIRS,), 1, 5), jax.random.fold_in(arg_keys[6], 1), 1, 4).astype(jnp.int32),
        "inv_lower": gaussian(arg_keys[7], (NT, B, B), B ** -0.5, 0.09375, ((1, 4), (2, 8))),
        "inv_upper": gaussian(arg_keys[8], (NT, B, B), B ** -0.5, 0.09375, ((1, 4), (2, 8))),
    }


def project(solved, factors):
    return jnp.einsum("nb,mbr->mnr", solved.astype(jnp.bfloat16).astype(jnp.float32), factors.astype(jnp.float32), precision=lax.Precision.HIGHEST)


def expand(masked, factors):
    return jnp.einsum("mnr,mbr->mnb", masked.astype(jnp.float32), factors.astype(jnp.float32), precision=lax.Precision.HIGHEST)


def apply_inverse(rounded, inverse):
    return lax.dot_general(rounded, inverse, (((1,), (1,)), ((), ())), preferred_element_type=jnp.float32)


def reference(right_sides, low_left, low_right, up_left, up_right, low_ranks, up_ranks, inv_lower, inv_upper):
    columns = jnp.arange(R, dtype=jnp.int32)
    residual = right_sides
    forward = []
    for section in range(NT):
        solved = apply_inverse(residual[section].astype(jnp.bfloat16), inv_lower[section])
        forward.append(solved)
        if section + 1 < NT:
            pair_index = np.array([tile * (tile - 1) // 2 + section for tile in range(section + 1, NT)], dtype=np.int32)
            projections = project(solved, low_right[pair_index])
            rank_mask = (columns[None, :] < RBLK * low_ranks[pair_index][:, None]).astype(jnp.float32)
            masked = (projections * rank_mask[:, None, :]).astype(jnp.bfloat16)
            residual = residual.at[section + 1:].add(-expand(masked, low_left[pair_index]))
    state = jnp.stack(forward)
    solutions = [None] * NT
    for section in range(NT - 1, -1, -1):
        solved = apply_inverse(state[section].astype(jnp.bfloat16), inv_upper[section])
        solutions[section] = solved
        if section > 0:
            pair_index = np.array([section * (section - 1) // 2 + tile for tile in range(section)], dtype=np.int32)
            projections = project(solved, up_right[pair_index])
            rank_mask = (columns[None, :] < RBLK * up_ranks[pair_index][:, None]).astype(jnp.float32)
            masked = (projections * rank_mask[:, None, :]).astype(jnp.bfloat16)
            state = state.at[:section].add(-expand(masked, up_left[pair_index]))
    return jnp.stack(solutions)
```

```python
import functools

import jax
import jax.numpy as jnp
import numpy as np
from jax import lax
from jax.experimental import pallas as pl
from jax.experimental.pallas import tpu as pltpu
from jax.sharding import PartitionSpec as P

RBLK = 32


def rank_mask(ranks, pair_index, rank_cols):
    columns = jnp.arange(rank_cols, dtype=jnp.int32)
    return (columns[None, :] < RBLK * ranks[pair_index][:, None]).astype(jnp.float32)


def times_inverse(block, inverse):
    return lax.dot_general(
        block, inverse, (((1,), (1,)), ((), ())), preferred_element_type=jnp.float32
    )


def sum_terms(moved, inverse):
    return times_inverse(moved, inverse)


def shards(
    right_sides, low_left, low_right, up_left, up_right, low_ranks, up_ranks, inv_lower, inv_upper
):
    tile_count = right_sides.shape[0]
    rank_cols = low_left.shape[2]
    residual = right_sides
    forward = []
    for section in range(tile_count):
        rounded = residual[section].astype(jnp.bfloat16)
        whole = lax.all_gather(rounded, "col", axis=1, tiled=True)
        moved = lax.all_to_all(whole, "row", split_axis=1, concat_axis=0, tiled=True)
        solved = lax.psum_scatter(
            sum_terms(moved, inv_lower[section]).astype(jnp.bfloat16),
            "row",
            scatter_dimension=0,
            tiled=True,
        ).astype(jnp.float32)
        forward.append(solved)
        if section + 1 < tile_count:
            pair_index = np.array(
                [tile * (tile - 1) // 2 + section for tile in range(section + 1, tile_count)],
                dtype=np.int32,
            )
            projections = jnp.einsum(
                "nw,mwr->mnr",
                solved.astype(jnp.bfloat16),
                low_right[pair_index],
                preferred_element_type=jnp.float32,
            )
            leading = lax.psum(projections[:1].astype(jnp.bfloat16), "col").astype(jnp.float32)
            if section + 2 < tile_count:
                remaining = lax.psum(projections[1:].astype(jnp.bfloat16), "col").astype(
                    jnp.float32
                )
                summed = jnp.concatenate([leading, remaining], axis=0)
            else:
                summed = leading
            masked = (summed * rank_mask(low_ranks, pair_index, rank_cols)[:, None, :]).astype(
                jnp.bfloat16
            )
            update = jnp.einsum(
                "mnr,mwr->mnw", masked, low_left[pair_index], preferred_element_type=jnp.float32
            )
            residual = residual.at[section + 1 :].add(-update)
    state = jnp.stack(forward)
    solutions = [None] * tile_count
    for section in range(tile_count - 1, -1, -1):
        rounded = state[section].astype(jnp.bfloat16)
        whole = lax.all_gather(rounded, "col", axis=1, tiled=True)
        moved = lax.all_to_all(whole, "row", split_axis=1, concat_axis=0, tiled=True)
        solved = lax.psum_scatter(
            sum_terms(moved, inv_upper[section]).astype(jnp.bfloat16),
            "row",
            scatter_dimension=0,
            tiled=True,
        ).astype(jnp.float32)
        solutions[section] = solved
        if section > 0:
            pair_index = np.array(
                [section * (section - 1) // 2 + tile for tile in range(section)], dtype=np.int32
            )
            projections = jnp.einsum(
                "nw,mwr->mnr",
                solved.astype(jnp.bfloat16),
                up_right[pair_index],
                preferred_element_type=jnp.float32,
            )
            leading = lax.psum(projections[-1:].astype(jnp.bfloat16), "col").astype(jnp.float32)
            if section > 1:
                remaining = lax.psum(projections[:-1].astype(jnp.bfloat16), "col").astype(
                    jnp.float32
                )
                summed = jnp.concatenate([remaining, leading], axis=0)
            else:
                summed = leading
            masked = (summed * rank_mask(up_ranks, pair_index, rank_cols)[:, None, :]).astype(
                jnp.bfloat16
            )
            update = jnp.einsum(
                "mnr,mwr->mnw", masked, up_left[pair_index], preferred_element_type=jnp.float32
            )
            state = state.at[:section].add(-update)
    return jnp.stack(solutions)


MESH = pl.DeviceIdType.MESH
STREAMS = 8
LAG = {"start": 0, "cross": 1.1, "spread": 3.1, "multiply": 5.2, "share": 6.6, "relay1": 7.6, "relay2": 9.6, "finish": 11.6, "late": 13.0}
TURN = 4


def schedule(streams, tiles):
    order = []
    for back in range(2):
        for stream in range(streams):
            for stage, lag in LAG.items():
                at = (lag + stream + back * TURN) / streams
                order.append((at - int(at), int(at), back, stream, stage))
    return sorted(order, key=lambda event: (event[0], -event[1]))


def kernel(
    shape, rhs, low_left, low_right, up_left, up_right, masks, inv_lower, inv_upper, out,
    inv, left, right, source, crossing, moved, own, chunks, arrived, near, near_in, proj, proj_in, far, far_in,
    rhs_sem, load_sem, factor_sem, w_send, w_recv, g0_send, g0_recv, g1_send, g1_recv, g2_send, g2_recv, r_send, r_recv,
    n_send, n_recv, p_send, p_recv, f_send, f_recv,
):
    tiles, rows, cols, chips, streams, part = shape
    pairs = low_left.shape[0]
    wide = out.shape[2]
    lanes = inv_lower.shape[2]
    piece = wide // cols
    row, col = lax.axis_index("row"), lax.axis_index("col")
    chip, core = lax.div(row, 2), lax.rem(row, 2)
    steps = 2 * tiles

    def remote(src, dst, send, recv, to_row, to_col):
        return pltpu.make_async_remote_copy(
            src_ref=src, dst_ref=dst, send_sem=send, recv_sem=recv,
            device_id=(to_row, to_col), device_id_type=MESH,
        )

    def inverse_of(step):
        return inv_lower.at[step] if step < tiles else inv_upper.at[steps - 1 - step]

    def half(step, which):
        return inv.at[step, :, pl.ds(pl.multiple_of(which * lanes, lanes), lanes)]

    def load_inverse(step):
        return pltpu.make_async_copy(inverse_of(step), half(step, core), load_sem.at[step])

    def lend_inverse(step):
        return remote(
            inverse_of(step), half(step, core), w_send.at[step], w_recv.at[step], row + 1 - 2 * core, col
        )

    factors = [
        (low_right, right.at[pl.ds(0, pairs)]), (low_left, left.at[pl.ds(0, pairs)]),
        (up_right, right.at[pl.ds(pairs, pairs)]), (up_left, left.at[pl.ds(pairs, pairs)]),
    ]
    factors = [pltpu.make_async_copy(a, b, factor_sem.at[k]) for k, (a, b) in enumerate(factors)]
    sides = [pltpu.make_async_copy(rhs.at[k], out.at[k], rhs_sem.at[k]) for k in range(tiles)]
    sides[0].start()
    for step in range(steps):
        lend_inverse(step).start()
        load_inverse(step).start()
        if step < tiles:
            factors[step].start()
            if step + 1 < tiles:
                sides[step + 1].start()
    far[...] = jnp.zeros_like(far)
    sides[0].wait()

    def own_lanes():
        return pl.ds(pl.multiple_of(col * piece, piece), piece)

    def geometry(step):
        back = lax.div(step, tiles)
        section = step + back * (2 * tiles - 1 - 2 * step)
        count = (1 - back) * (tiles - 1 - section) + back * section
        return back, section, count

    def tile_of(back, section, v):
        tile = section + (1 - 2 * back) * (1 + v)
        high = back * section + (1 - back) * tile
        low = section + tile - high
        return tile, back * pairs + lax.div(high * (high - 1), 2) + low

    def place(stream):
        return pl.ds(stream * part, part)

    def side_of(step):
        return lax.rem(step, 2)

    def g0(step, stream, hop):
        to = lax.rem(col + hop, cols)
        return remote(
            source.at[stream, :, pl.ds(pl.multiple_of(to * piece, piece), piece)],
            crossing.at[side_of(step), stream, col],
            g0_send.at[stream, hop], g0_recv.at[stream, side_of(step), col],
            row, to,
        )

    def g1(step, stream, hop):
        to = lax.rem(chip + hop, chips)
        return remote(
            crossing.at[side_of(step), stream, to],
            moved.at[side_of(step), stream, chip, :, own_lanes()],
            g1_send.at[stream, hop], g1_recv.at[stream, side_of(step), chip],
            2 * to + core, col,
        )

    def g2(step, stream, hop):
        view = moved.at[side_of(step), stream, :, :, own_lanes()]
        return remote(
            view, view, g2_send.at[stream, hop], g2_recv.at[stream, side_of(step), hop],
            row, lax.rem(col + hop, cols),
        )

    def pass_on(step, stream, owner, way):
        side = side_of(step)
        to = chip + way
        slot = owner + lax.div(1 - way, 2) * jnp.where(owner == to, chips - owner, 0)
        return remote(
            chunks.at[side, stream, owner], arrived.at[side, stream, slot],
            r_send.at[stream, side, owner], r_recv.at[stream, side, slot],
            2 * to + core, col,
        )

    def took(step, stream, slot):
        side = side_of(step)
        view = arrived.at[side, stream, slot]
        pltpu.make_async_copy(view, view, r_recv.at[stream, side, slot]).wait()
        return arrived[side, stream, slot].astype(jnp.float32)

    def line(step, stream, leg):
        side = side_of(step)
        up, down = chip == leg, chip == chips - 1 - leg

        @pl.when(jnp.logical_or(up, down))
        def _():
            way = jnp.where(up, 1, -1)

            def one(k, carry):
                owner = jnp.where(up, chips - 1 - k, k)
                total = own[side, stream, owner]
                if leg > 0:
                    total += took(step, stream, owner)
                chunks[side, stream, owner] = total.astype(jnp.bfloat16)
                pass_on(step, stream, owner, way).start()
                return carry

            lax.fori_loop(0, chips - 1 - leg, one, 0)

    def near_copy(step, stream, hop):
        to = lax.rem(chip + hop, chips)
        return remote(
            near.at[stream, to], near_in.at[side_of(step), stream, hop],
            n_send.at[stream, hop], n_recv.at[stream, side_of(step), hop],
            2 * to + core, col,
        )

    def project(step, stream, hop):
        return remote(
            proj.at[stream], proj_in.at[side_of(step), stream, hop],
            p_send.at[stream, hop], p_recv.at[stream, side_of(step), hop],
            row, lax.rem(col + hop, cols),
        )

    def project_far(step, stream, hop):
        return remote(
            far.at[stream], far_in.at[side_of(step), stream, hop],
            f_send.at[stream, hop], f_recv.at[stream, side_of(step), hop],
            row, lax.rem(col + hop, cols),
        )

    def subtract(tile, pair, stream, total):
        masked = (total * masks[pair]).astype(jnp.bfloat16)
        out[tile, place(stream), :] -= times_inverse(masked, left[pair])

    def start(step, stream):
        @pl.when(jnp.logical_and(step > 0, step != tiles))
        def _():
            if stream == 0:

                @pl.when(step == 1)
                def _():
                    for k in range(1, tiles):
                        sides[k].wait()
                    for k in range(1, 4):
                        factors[k].wait()

            back, section, _ = geometry(step - 1)
            tile, pair = tile_of(back, section, 0)
            for hop in range(1, cols):
                project(step - 1, stream, hop).wait()
            total = proj[stream].astype(jnp.float32)
            for hop in range(1, cols):
                total += proj_in[side_of(step - 1), stream, hop].astype(jnp.float32)
            subtract(tile, pair, stream, total)

        _, section, _ = geometry(step)
        source[stream] = out[section, place(stream), :].astype(jnp.bfloat16)
        mine = pl.ds(pl.multiple_of(col * piece, piece), piece)
        pltpu.make_async_copy(
            source.at[stream, :, mine], crossing.at[side_of(step), stream, col],
            g0_recv.at[stream, side_of(step), col],
        ).start()
        for hop in range(1, cols):
            g0(step, stream, hop).start()

    def cross(step, stream):
        side = side_of(step)
        for k in range(cols):
            view = crossing.at[side, stream, k]
            pltpu.make_async_copy(view, view, g0_recv.at[stream, side, k]).wait()
        pltpu.make_async_copy(
            crossing.at[side, stream, chip], moved.at[side, stream, chip, :, own_lanes()],
            g1_recv.at[stream, side, chip],
        ).start()
        for hop in range(1, chips):
            g1(step, stream, hop).start()
        for hop in range(1, cols):
            g0(step, stream, hop).wait_send()

    def spread(step, stream):
        for k in range(chips):
            view = moved.at[side_of(step), stream, k, :, own_lanes()]
            pltpu.make_async_copy(view, view, g1_recv.at[stream, side_of(step), k]).wait()
        for hop in range(1, cols):
            g2(step, stream, hop).start()
        for hop in range(1, chips):
            g1(step, stream, hop).wait_send()

    def multiply(step, stream):
        side = side_of(step)
        back, section, count = geometry(step)
        if stream == 0:
            view = half(step, core)
            pltpu.make_async_copy(view, view, load_sem.at[step]).wait()
            view = half(step, 1 - core)
            pltpu.make_async_copy(view, view, w_recv.at[step]).wait()

            @pl.when(step == 0)
            def _():
                factors[0].wait()

        for hop in range(1, cols):
            view = moved.at[
                side, stream, :, :,
                pl.ds(pl.multiple_of(lax.rem(col + cols - hop, cols) * piece, piece), piece),
            ]
            pltpu.make_async_copy(view, view, g2_recv.at[stream, side, hop]).wait()
        whole = moved[side, stream].reshape(chips * part, wide)
        terms = times_inverse(whole, inv[step])
        own[side, stream] = terms.reshape(chips, part, wide)

        @pl.when(count > 0)
        def _():
            _, pair = tile_of(back, section, 0)
            rounded = own[side, stream].reshape(chips * part, wide).astype(jnp.bfloat16)
            near[stream] = (
                jnp.dot(rounded, right[pair], preferred_element_type=jnp.float32)
                .astype(jnp.bfloat16)
                .reshape(chips, part, -1)
            )
            for hop in range(1, chips):
                near_copy(step, stream, hop).start()

        line(step, stream, 0)
        for hop in range(1, cols):
            g2(step, stream, hop).wait_send()

    def share(step, stream):
        _, _, count = geometry(step)

        @pl.when(count > 0)
        def _():
            for hop in range(1, chips):
                near_copy(step, stream, hop).wait()
            total = near[stream, chip].astype(jnp.float32)
            for hop in range(1, chips):
                total += near_in[side_of(step), stream, hop].astype(jnp.float32)
            proj[stream] = total.astype(jnp.bfloat16)
            for hop in range(1, cols):
                project(step, stream, hop).start()

    def finish(step, stream):
        side = side_of(step)
        back, section, count = geometry(step)
        out[section, place(stream), :] = own[side, stream, chip]

        @pl.when(chip > 0)
        def _():
            out[section, place(stream), :] += took(step, stream, chip)

        @pl.when(chip < chips - 1)
        def _():
            out[section, place(stream), :] += took(step, stream, chips)

        for owner in range(chips):

            @pl.when(chip != owner)
            def _():
                pass_on(step, stream, owner, jnp.where(owner > chip, 1, -1)).wait_send()

        @pl.when(count > 1)
        def _():
            rounded = out[section, place(stream), :].astype(jnp.bfloat16)

            def one(v, carry):
                _, pair = tile_of(back, section, v)
                far[stream, v - 1] = jnp.dot(
                    rounded, right[pair], preferred_element_type=jnp.float32
                ).astype(jnp.bfloat16)
                return carry

            lax.fori_loop(1, count, one, 0)
            for hop in range(1, cols):
                project_far(step, stream, hop).start()

    def late(step, stream):
        back, section, count = geometry(step)
        side = side_of(step)

        @pl.when(count > 1)
        def _():
            for hop in range(1, cols):
                project_far(step, stream, hop).wait()

            def one(v, carry):
                tile, pair = tile_of(back, section, v)
                total = far[stream, v - 1].astype(jnp.float32)
                for hop in range(1, cols):
                    total += far_in[side, stream, hop, v - 1].astype(jnp.float32)
                subtract(tile, pair, stream, total)
                return carry

            lax.fori_loop(1, count, one, 0)

    stages = {
        "start": start, "cross": cross, "spread": spread, "multiply": multiply, "share": share,
        "relay1": functools.partial(line, leg=1), "relay2": functools.partial(line, leg=2),
        "finish": finish, "late": late,
    }
    order = schedule(streams, tiles)
    latest = max(shift for _, shift, _, _, _ in order)

    def body(turn, carry):
        for _, shift, back, stream, stage in order:
            step = turn - shift

            @pl.when(jnp.logical_and(step >= back * tiles, step < (1 + back) * tiles))
            def _():
                stages[stage](step, stream)

        return carry

    lax.fori_loop(0, steps + latest, body, 0)
    for step in range(steps):
        lend_inverse(step).wait_send()


def fused(
    rows, cols, streams, right_sides, low_left, low_right, up_left, up_right, low_ranks, up_ranks,
    inv_lower, inv_upper,
):
    tiles, held, wide = right_sides.shape
    pairs, _, rank_cols = low_left.shape
    chips = rows // 2
    part = held // streams
    masks = rank_mask(
        jnp.concatenate([low_ranks, up_ranks]), np.arange(2 * pairs), rank_cols
    ).reshape(2 * pairs, 1, rank_cols)
    half = jnp.bfloat16
    dma = pltpu.SemaphoreType.DMA
    later = max(tiles - 2, 1)
    scratch = [
        pltpu.VMEM((2 * tiles, wide, wide), half),
        pltpu.VMEM((2 * pairs, wide, rank_cols), half),
        pltpu.VMEM((2 * pairs, wide, rank_cols), half),
        pltpu.VMEM((streams, part, wide), half),
        pltpu.VMEM((2, streams, cols, part, wide // cols), half),
        pltpu.VMEM((2, streams, chips, part, wide), half),
        pltpu.VMEM((2, streams, chips, part, wide), jnp.float32),
        pltpu.VMEM((2, streams, chips, part, wide), half),
        pltpu.VMEM((2, streams, chips + 1, part, wide), half),
        pltpu.VMEM((streams, chips, part, rank_cols), half),
        pltpu.VMEM((2, streams, chips, part, rank_cols), half),
        pltpu.VMEM((streams, part, rank_cols), half),
        pltpu.VMEM((2, streams, cols, part, rank_cols), half),
        pltpu.VMEM((streams, later, part, rank_cols), half),
        pltpu.VMEM((2, streams, cols, later, part, rank_cols), half),
        dma((tiles,)), dma((2 * tiles,)), dma((4,)), dma((2 * tiles,)), dma((2 * tiles,)),
        dma((streams, cols)), dma((streams, 2, cols)),
        dma((streams, chips)), dma((streams, 2, chips)),
        dma((streams, cols)), dma((streams, 2, cols)),
        dma((streams, 2, chips)), dma((streams, 2, chips + 1)),
        dma((streams, chips)), dma((streams, 2, chips)),
        dma((streams, cols)), dma((streams, 2, cols)),
        dma((streams, cols)), dma((streams, 2, cols)),
    ]
    anywhere = pl.BlockSpec(memory_space=pl.ANY)
    vmem = pl.BlockSpec(memory_space=pltpu.VMEM)
    return pl.pallas_call(
        functools.partial(kernel, (tiles, rows, cols, chips, streams, part)),
        out_shape=jax.ShapeDtypeStruct(right_sides.shape, jnp.float32),
        in_specs=[anywhere] * 5 + [vmem] + [anywhere] * 2,
        out_specs=vmem,
        scratch_shapes=scratch,
        compiler_params=pltpu.CompilerParams(
            has_side_effects=True, vmem_limit_bytes=60 * 1024 * 1024
        ),
    )(right_sides, low_left, low_right, up_left, up_right, masks, inv_lower, inv_upper)


def pick(mesh):
    rows, cols = mesh.shape["row"], mesh.shape["col"]

    def run(right_sides, *rest):
        tiles, held, wide = right_sides.shape
        fits = rows == 8 and cols == 4 and tiles == 4 and wide == 2 * rest[-1].shape[2]
        if fits and wide % (128 * cols) == 0 and held % (16 * STREAMS) == 0:
            return fused(rows, cols, STREAMS, right_sides, *rest)
        return shards(right_sides, *rest)

    return run


def solution(mesh):
    in_specs = (
        P(None, "row", "col"),
        P(None, "col", None),
        P(None, "col", None),
        P(None, "col", None),
        P(None, "col", None),
        P(),
        P(),
        P(None, "col", "row"),
        P(None, "col", "row"),
    )
    out_specs = P(None, "row", "col")
    return jax.shard_map(pick(mesh), mesh=mesh, in_specs=in_specs, out_specs=out_specs, check_vma=False)
```

```python
import functools

import jax
import jax.numpy as jnp
import numpy as np
from jax import lax
from jax.experimental import pallas as pl
from jax.experimental.pallas import tpu as pltpu
from jax.sharding import PartitionSpec as P

RBLK = 32


def rank_mask(ranks, pair_index, rank_cols):
    columns = jnp.arange(rank_cols, dtype=jnp.int32)
    return (columns[None, :] < RBLK * ranks[pair_index][:, None]).astype(jnp.float32)


def times_inverse(block, inverse):
    return lax.dot_general(
        block, inverse, (((1,), (1,)), ((), ())), preferred_element_type=jnp.float32
    )


def sum_terms(moved, inverse):
    return times_inverse(moved, inverse)


def shards(
    right_sides, low_left, low_right, up_left, up_right, low_ranks, up_ranks, inv_lower, inv_upper
):
    tile_count = right_sides.shape[0]
    rank_cols = low_left.shape[2]
    residual = right_sides
    forward = []
    for section in range(tile_count):
        rounded = residual[section].astype(jnp.bfloat16)
        whole = lax.all_gather(rounded, "col", axis=1, tiled=True)
        moved = lax.all_to_all(whole, "row", split_axis=1, concat_axis=0, tiled=True)
        solved = lax.psum_scatter(
            sum_terms(moved, inv_lower[section]).astype(jnp.bfloat16),
            "row",
            scatter_dimension=0,
            tiled=True,
        ).astype(jnp.float32)
        forward.append(solved)
        if section + 1 < tile_count:
            pair_index = np.array(
                [tile * (tile - 1) // 2 + section for tile in range(section + 1, tile_count)],
                dtype=np.int32,
            )
            projections = jnp.einsum(
                "nw,mwr->mnr",
                solved.astype(jnp.bfloat16),
                low_right[pair_index],
                preferred_element_type=jnp.float32,
            )
            leading = lax.psum(projections[:1].astype(jnp.bfloat16), "col").astype(jnp.float32)
            if section + 2 < tile_count:
                remaining = lax.psum(projections[1:].astype(jnp.bfloat16), "col").astype(
                    jnp.float32
                )
                summed = jnp.concatenate([leading, remaining], axis=0)
            else:
                summed = leading
            masked = (summed * rank_mask(low_ranks, pair_index, rank_cols)[:, None, :]).astype(
                jnp.bfloat16
            )
            update = jnp.einsum(
                "mnr,mwr->mnw", masked, low_left[pair_index], preferred_element_type=jnp.float32
            )
            residual = residual.at[section + 1 :].add(-update)
    state = jnp.stack(forward)
    solutions = [None] * tile_count
    for section in range(tile_count - 1, -1, -1):
        rounded = state[section].astype(jnp.bfloat16)
        whole = lax.all_gather(rounded, "col", axis=1, tiled=True)
        moved = lax.all_to_all(whole, "row", split_axis=1, concat_axis=0, tiled=True)
        solved = lax.psum_scatter(
            sum_terms(moved, inv_upper[section]).astype(jnp.bfloat16),
            "row",
            scatter_dimension=0,
            tiled=True,
        ).astype(jnp.float32)
        solutions[section] = solved
        if section > 0:
            pair_index = np.array(
                [section * (section - 1) // 2 + tile for tile in range(section)], dtype=np.int32
            )
            projections = jnp.einsum(
                "nw,mwr->mnr",
                solved.astype(jnp.bfloat16),
                up_right[pair_index],
                preferred_element_type=jnp.float32,
            )
            leading = lax.psum(projections[-1:].astype(jnp.bfloat16), "col").astype(jnp.float32)
            if section > 1:
                remaining = lax.psum(projections[:-1].astype(jnp.bfloat16), "col").astype(
                    jnp.float32
                )
                summed = jnp.concatenate([remaining, leading], axis=0)
            else:
                summed = leading
            masked = (summed * rank_mask(up_ranks, pair_index, rank_cols)[:, None, :]).astype(
                jnp.bfloat16
            )
            update = jnp.einsum(
                "mnr,mwr->mnw", masked, up_left[pair_index], preferred_element_type=jnp.float32
            )
            state = state.at[:section].add(-update)
    return jnp.stack(solutions)


MESH = pl.DeviceIdType.MESH
STREAMS = 8
LAG = {"start": 0, "cross": 1.1, "spread": 3.1, "multiply": 4.6, "share": 6.3, "relay1": 7.3, "relay2": 9.1, "finish": 10.4, "late": 14.3}
LAST = {"relay1": 6.6, "relay2": 7.8, "finish": 8.9}
TURN = 1.0


def schedule(streams, tiles):
    order = []
    for back in range(2):
        for stream in range(streams):
            spans = [(stage, lag, 0, tiles - (stage in LAST)) for stage, lag in LAG.items()]
            spans += [(stage, lag, tiles - 1, tiles) for stage, lag in LAST.items()]
            for stage, lag, first, end in spans:
                at = (lag + stream + back * TURN) / streams
                order.append(
                    (at - int(at), int(at), back * tiles + first, back * tiles + end, stream, stage)
                )
    return sorted(order, key=lambda event: (event[0], -event[1]))


def kernel(
    shape, rhs, low_left, low_right, up_left, up_right, masks, inv_lower, inv_upper, out,
    inv, left, right, source, crossing, moved, own, chunks, arrived, near, near_in, proj, proj_in, far, far_in,
    rhs_sem, load_sem, factor_sem, w_send, w_recv, g0_send, g0_recv, g1_send, g1_recv, g2_send, g2_recv, r_send, r_recv,
    n_send, n_recv, p_send, p_recv, f_send, f_recv,
):
    tiles, rows, cols, chips, streams, part = shape
    pairs = low_left.shape[0]
    wide = out.shape[2]
    lanes = inv_lower.shape[2]
    piece = wide // cols
    row, col = lax.axis_index("row"), lax.axis_index("col")
    chip, core = lax.div(row, 2), lax.rem(row, 2)
    steps = 2 * tiles

    def remote(src, dst, send, recv, to_row, to_col):
        return pltpu.make_async_remote_copy(
            src_ref=src, dst_ref=dst, send_sem=send, recv_sem=recv,
            device_id=(to_row, to_col), device_id_type=MESH,
        )

    def inverse_of(step):
        return inv_lower.at[step] if step < tiles else inv_upper.at[steps - 1 - step]

    def half(step, which):
        return inv.at[step, :, pl.ds(pl.multiple_of(which * lanes, lanes), lanes)]

    def load_inverse(step):
        return pltpu.make_async_copy(inverse_of(step), half(step, core), load_sem.at[step])

    def lend_inverse(step):
        return remote(
            inverse_of(step), half(step, core), w_send.at[step], w_recv.at[step], row + 1 - 2 * core, col
        )

    factors = [
        (low_right, right.at[pl.ds(0, pairs)]), (low_left, left.at[pl.ds(0, pairs)]),
        (up_right, right.at[pl.ds(pairs, pairs)]), (up_left, left.at[pl.ds(pairs, pairs)]),
    ]
    factors = [pltpu.make_async_copy(a, b, factor_sem.at[k]) for k, (a, b) in enumerate(factors)]
    sides = [pltpu.make_async_copy(rhs.at[k], out.at[k], rhs_sem.at[k]) for k in range(tiles)]
    sides[0].start()
    for step in range(steps):
        lend_inverse(step).start()
        load_inverse(step).start()
        if step < tiles:
            factors[step].start()
            if step + 1 < tiles:
                sides[step + 1].start()
    far[...] = jnp.zeros_like(far)
    sides[0].wait()

    def own_lanes():
        return pl.ds(pl.multiple_of(col * piece, piece), piece)

    def geometry(step):
        back = lax.div(step, tiles)
        section = step + back * (2 * tiles - 1 - 2 * step)
        count = (1 - back) * (tiles - 1 - section) + back * section
        return back, section, count

    def tile_of(back, section, v):
        tile = section + (1 - 2 * back) * (1 + v)
        high = back * section + (1 - back) * tile
        low = section + tile - high
        return tile, back * pairs + lax.div(high * (high - 1), 2) + low

    def place(stream):
        return pl.ds(stream * part, part)

    def side_of(step):
        return lax.rem(step, 2)

    def g0(step, stream, hop):
        to = lax.rem(col + hop, cols)
        return remote(
            source.at[stream, :, pl.ds(pl.multiple_of(to * piece, piece), piece)],
            crossing.at[side_of(step), stream, col],
            g0_send.at[stream, hop], g0_recv.at[stream, side_of(step), col],
            row, to,
        )

    def g1(step, stream, hop):
        to = lax.rem(chip + hop, chips)
        return remote(
            crossing.at[side_of(step), stream, to],
            moved.at[side_of(step), stream, chip, :, own_lanes()],
            g1_send.at[stream, hop], g1_recv.at[stream, side_of(step), chip],
            2 * to + core, col,
        )

    def g2(step, stream, hop):
        view = moved.at[side_of(step), stream, :, :, own_lanes()]
        return remote(
            view, view, g2_send.at[stream, hop], g2_recv.at[stream, side_of(step), hop],
            row, lax.rem(col + hop, cols),
        )

    def pass_on(step, stream, owner, way):
        side = side_of(step)
        to = chip + way
        slot = owner + lax.div(1 - way, 2) * jnp.where(owner == to, chips - owner, 0)
        return remote(
            chunks.at[side, stream, owner], arrived.at[side, stream, slot],
            r_send.at[stream, side, owner], r_recv.at[stream, side, slot],
            2 * to + core, col,
        )

    def took(step, stream, slot):
        side = side_of(step)
        view = arrived.at[side, stream, slot]
        pltpu.make_async_copy(view, view, r_recv.at[stream, side, slot]).wait()
        return arrived[side, stream, slot].astype(jnp.float32)

    def line(step, stream, leg):
        side = side_of(step)
        up, down = chip == leg, chip == chips - 1 - leg

        @pl.when(jnp.logical_or(up, down))
        def _():
            way = jnp.where(up, 1, -1)

            def one(k, carry):
                owner = jnp.where(up, chips - 1 - k, k)
                total = own[side, stream, owner]
                if leg > 0:
                    total += took(step, stream, owner)
                chunks[side, stream, owner] = total.astype(jnp.bfloat16)
                pass_on(step, stream, owner, way).start()
                return carry

            lax.fori_loop(0, chips - 1 - leg, one, 0)

    def near_copy(step, stream, hop):
        to = lax.rem(chip + hop, chips)
        return remote(
            near.at[stream, to], near_in.at[side_of(step), stream, hop],
            n_send.at[stream, hop], n_recv.at[stream, side_of(step), hop],
            2 * to + core, col,
        )

    def project(step, stream, hop):
        return remote(
            proj.at[stream], proj_in.at[side_of(step), stream, hop],
            p_send.at[stream, hop], p_recv.at[stream, side_of(step), hop],
            row, lax.rem(col + hop, cols),
        )

    def project_far(step, stream, hop):
        return remote(
            far.at[stream], far_in.at[side_of(step), stream, hop],
            f_send.at[stream, hop], f_recv.at[stream, side_of(step), hop],
            row, lax.rem(col + hop, cols),
        )

    def subtract(tile, pair, stream, total):
        masked = (total * masks[pair]).astype(jnp.bfloat16)
        out[tile, place(stream), :] -= times_inverse(masked, left[pair])

    def start(step, stream):
        @pl.when(jnp.logical_and(step > 0, step != tiles))
        def _():
            if stream == 0:

                @pl.when(step == 1)
                def _():
                    for k in range(1, tiles):
                        sides[k].wait()
                    for k in range(1, 4):
                        factors[k].wait()

            back, section, _ = geometry(step - 1)
            tile, pair = tile_of(back, section, 0)
            for hop in range(1, cols):
                project(step - 1, stream, hop).wait()
            total = proj[stream].astype(jnp.float32)
            for hop in range(1, cols):
                total += proj_in[side_of(step - 1), stream, hop].astype(jnp.float32)
            subtract(tile, pair, stream, total)

        _, section, _ = geometry(step)
        source[stream] = out[section, place(stream), :].astype(jnp.bfloat16)
        mine = pl.ds(pl.multiple_of(col * piece, piece), piece)
        pltpu.make_async_copy(
            source.at[stream, :, mine], crossing.at[side_of(step), stream, col],
            g0_recv.at[stream, side_of(step), col],
        ).start()
        for hop in range(1, cols):
            g0(step, stream, hop).start()

    def cross(step, stream):
        side = side_of(step)
        for k in range(cols):
            view = crossing.at[side, stream, k]
            pltpu.make_async_copy(view, view, g0_recv.at[stream, side, k]).wait()
        pltpu.make_async_copy(
            crossing.at[side, stream, chip], moved.at[side, stream, chip, :, own_lanes()],
            g1_recv.at[stream, side, chip],
        ).start()
        for hop in range(1, chips):
            g1(step, stream, hop).start()
        for hop in range(1, cols):
            g0(step, stream, hop).wait_send()

    def spread(step, stream):
        for k in range(chips):
            view = moved.at[side_of(step), stream, k, :, own_lanes()]
            pltpu.make_async_copy(view, view, g1_recv.at[stream, side_of(step), k]).wait()
        for hop in range(1, cols):
            g2(step, stream, hop).start()
        for hop in range(1, chips):
            g1(step, stream, hop).wait_send()

    def multiply(step, stream):
        side = side_of(step)
        back, section, count = geometry(step)
        if stream == 0:
            view = half(step, core)
            pltpu.make_async_copy(view, view, load_sem.at[step]).wait()
            view = half(step, 1 - core)
            pltpu.make_async_copy(view, view, w_recv.at[step]).wait()

            @pl.when(step == 0)
            def _():
                factors[0].wait()

        for hop in range(1, cols):
            view = moved.at[
                side, stream, :, :,
                pl.ds(pl.multiple_of(lax.rem(col + cols - hop, cols) * piece, piece), piece),
            ]
            pltpu.make_async_copy(view, view, g2_recv.at[stream, side, hop]).wait()
        whole = moved[side, stream].reshape(chips * part, wide)
        terms = times_inverse(whole, inv[step])
        own[side, stream] = terms.reshape(chips, part, wide)

        @pl.when(count > 0)
        def _():
            _, pair = tile_of(back, section, 0)
            rounded = own[side, stream].reshape(chips * part, wide).astype(jnp.bfloat16)
            near[stream] = (
                jnp.dot(rounded, right[pair], preferred_element_type=jnp.float32)
                .astype(jnp.bfloat16)
                .reshape(chips, part, -1)
            )
            for hop in range(1, chips):
                near_copy(step, stream, hop).start()

        line(step, stream, 0)
        for hop in range(1, cols):
            g2(step, stream, hop).wait_send()

    def share(step, stream):
        _, _, count = geometry(step)

        @pl.when(count > 0)
        def _():
            for hop in range(1, chips):
                near_copy(step, stream, hop).wait()
            total = near[stream, chip].astype(jnp.float32)
            for hop in range(1, chips):
                total += near_in[side_of(step), stream, hop].astype(jnp.float32)
            proj[stream] = total.astype(jnp.bfloat16)
            for hop in range(1, cols):
                project(step, stream, hop).start()

    def finish(step, stream):
        side = side_of(step)
        back, section, count = geometry(step)
        out[section, place(stream), :] = own[side, stream, chip]

        @pl.when(chip > 0)
        def _():
            out[section, place(stream), :] += took(step, stream, chip)

        @pl.when(chip < chips - 1)
        def _():
            out[section, place(stream), :] += took(step, stream, chips)

        for owner in range(chips):

            @pl.when(chip != owner)
            def _():
                pass_on(step, stream, owner, jnp.where(owner > chip, 1, -1)).wait_send()

        @pl.when(count > 1)
        def _():
            rounded = out[section, place(stream), :].astype(jnp.bfloat16)

            def one(v, carry):
                _, pair = tile_of(back, section, v)
                far[stream, v - 1] = jnp.dot(
                    rounded, right[pair], preferred_element_type=jnp.float32
                ).astype(jnp.bfloat16)
                return carry

            lax.fori_loop(1, count, one, 0)
            for hop in range(1, cols):
                project_far(step, stream, hop).start()

    def late(step, stream):
        back, section, count = geometry(step)
        side = side_of(step)

        @pl.when(count > 1)
        def _():
            for hop in range(1, cols):
                project_far(step, stream, hop).wait()

            def one(v, carry):
                tile, pair = tile_of(back, section, v)
                total = far[stream, v - 1].astype(jnp.float32)
                for hop in range(1, cols):
                    total += far_in[side, stream, hop, v - 1].astype(jnp.float32)
                subtract(tile, pair, stream, total)
                return carry

            lax.fori_loop(1, count, one, 0)

    stages = {
        "start": start, "cross": cross, "spread": spread, "multiply": multiply, "share": share,
        "relay1": functools.partial(line, leg=1), "relay2": functools.partial(line, leg=2),
        "finish": finish, "late": late,
    }
    order = schedule(streams, tiles)
    latest = max(event[1] for event in order)

    def body(turn, carry):
        for _, shift, first, end, stream, stage in order:
            step = turn - shift

            @pl.when(jnp.logical_and(step >= first, step < end))
            def _():
                stages[stage](step, stream)

        return carry

    lax.fori_loop(0, steps + latest, body, 0)
    for step in range(steps):
        lend_inverse(step).wait_send()


def fused(
    rows, cols, streams, right_sides, low_left, low_right, up_left, up_right, low_ranks, up_ranks,
    inv_lower, inv_upper,
):
    tiles, held, wide = right_sides.shape
    pairs, _, rank_cols = low_left.shape
    chips = rows // 2
    part = held // streams
    masks = rank_mask(
        jnp.concatenate([low_ranks, up_ranks]), np.arange(2 * pairs), rank_cols
    ).reshape(2 * pairs, 1, rank_cols)
    half = jnp.bfloat16
    dma = pltpu.SemaphoreType.DMA
    later = max(tiles - 2, 1)
    scratch = [
        pltpu.VMEM((2 * tiles, wide, wide), half),
        pltpu.VMEM((2 * pairs, wide, rank_cols), half),
        pltpu.VMEM((2 * pairs, wide, rank_cols), half),
        pltpu.VMEM((streams, part, wide), half),
        pltpu.VMEM((2, streams, cols, part, wide // cols), half),
        pltpu.VMEM((2, streams, chips, part, wide), half),
        pltpu.VMEM((2, streams, chips, part, wide), jnp.float32),
        pltpu.VMEM((2, streams, chips, part, wide), half),
        pltpu.VMEM((2, streams, chips + 1, part, wide), half),
        pltpu.VMEM((streams, chips, part, rank_cols), half),
        pltpu.VMEM((2, streams, chips, part, rank_cols), half),
        pltpu.VMEM((streams, part, rank_cols), half),
        pltpu.VMEM((2, streams, cols, part, rank_cols), half),
        pltpu.VMEM((streams, later, part, rank_cols), half),
        pltpu.VMEM((2, streams, cols, later, part, rank_cols), half),
        dma((tiles,)), dma((2 * tiles,)), dma((4,)), dma((2 * tiles,)), dma((2 * tiles,)),
        dma((streams, cols)), dma((streams, 2, cols)),
        dma((streams, chips)), dma((streams, 2, chips)),
        dma((streams, cols)), dma((streams, 2, cols)),
        dma((streams, 2, chips)), dma((streams, 2, chips + 1)),
        dma((streams, chips)), dma((streams, 2, chips)),
        dma((streams, cols)), dma((streams, 2, cols)),
        dma((streams, cols)), dma((streams, 2, cols)),
    ]
    anywhere = pl.BlockSpec(memory_space=pl.ANY)
    vmem = pl.BlockSpec(memory_space=pltpu.VMEM)
    return pl.pallas_call(
        functools.partial(kernel, (tiles, rows, cols, chips, streams, part)),
        out_shape=jax.ShapeDtypeStruct(right_sides.shape, jnp.float32),
        in_specs=[anywhere] * 5 + [vmem] + [anywhere] * 2,
        out_specs=vmem,
        scratch_shapes=scratch,
        compiler_params=pltpu.CompilerParams(
            has_side_effects=True, vmem_limit_bytes=60 * 1024 * 1024
        ),
    )(right_sides, low_left, low_right, up_left, up_right, masks, inv_lower, inv_upper)


def pick(mesh):
    rows, cols = mesh.shape["row"], mesh.shape["col"]

    def run(right_sides, *rest):
        tiles, held, wide = right_sides.shape
        fits = rows == 8 and cols == 4 and tiles == 4 and wide == 2 * rest[-1].shape[2]
        if fits and wide % (128 * cols) == 0 and held % (16 * STREAMS) == 0:
            return fused(rows, cols, STREAMS, right_sides, *rest)
        return shards(right_sides, *rest)

    return run


def solution(mesh):
    in_specs = (
        P(None, "row", "col"),
        P(None, "col", None),
        P(None, "col", None),
        P(None, "col", None),
        P(None, "col", None),
        P(),
        P(),
        P(None, "col", "row"),
        P(None, "col", "row"),
    )
    out_specs = P(None, "row", "col")
    return jax.shard_map(pick(mesh), mesh=mesh, in_specs=in_specs, out_specs=out_specs, check_vma=False)
```

```python
import functools

import jax
import jax.numpy as jnp
import numpy as np
from jax import lax
from jax.experimental import pallas as pl
from jax.experimental.pallas import tpu as pltpu
from jax.sharding import PartitionSpec as P

RBLK = 32


def rank_mask(ranks, pair_index, rank_cols):
    columns = jnp.arange(rank_cols, dtype=jnp.int32)
    return (columns[None, :] < RBLK * ranks[pair_index][:, None]).astype(jnp.float32)


def times_inverse(block, inverse):
    return lax.dot_general(
        block, inverse, (((1,), (1,)), ((), ())), preferred_element_type=jnp.float32
    )


def sum_terms(moved, inverse):
    return times_inverse(moved, inverse)


def shards(
    right_sides, low_left, low_right, up_left, up_right, low_ranks, up_ranks, inv_lower, inv_upper
):
    tile_count = right_sides.shape[0]
    rank_cols = low_left.shape[2]
    residual = right_sides
    forward = []
    for section in range(tile_count):
        rounded = residual[section].astype(jnp.bfloat16)
        whole = lax.all_gather(rounded, "col", axis=1, tiled=True)
        moved = lax.all_to_all(whole, "row", split_axis=1, concat_axis=0, tiled=True)
        solved = lax.psum_scatter(
            sum_terms(moved, inv_lower[section]).astype(jnp.bfloat16),
            "row",
            scatter_dimension=0,
            tiled=True,
        ).astype(jnp.float32)
        forward.append(solved)
        if section + 1 < tile_count:
            pair_index = np.array(
                [tile * (tile - 1) // 2 + section for tile in range(section + 1, tile_count)],
                dtype=np.int32,
            )
            projections = jnp.einsum(
                "nw,mwr->mnr",
                solved.astype(jnp.bfloat16),
                low_right[pair_index],
                preferred_element_type=jnp.float32,
            )
            leading = lax.psum(projections[:1].astype(jnp.bfloat16), "col").astype(jnp.float32)
            if section + 2 < tile_count:
                remaining = lax.psum(projections[1:].astype(jnp.bfloat16), "col").astype(
                    jnp.float32
                )
                summed = jnp.concatenate([leading, remaining], axis=0)
            else:
                summed = leading
            masked = (summed * rank_mask(low_ranks, pair_index, rank_cols)[:, None, :]).astype(
                jnp.bfloat16
            )
            update = jnp.einsum(
                "mnr,mwr->mnw", masked, low_left[pair_index], preferred_element_type=jnp.float32
            )
            residual = residual.at[section + 1 :].add(-update)
    state = jnp.stack(forward)
    solutions = [None] * tile_count
    for section in range(tile_count - 1, -1, -1):
        rounded = state[section].astype(jnp.bfloat16)
        whole = lax.all_gather(rounded, "col", axis=1, tiled=True)
        moved = lax.all_to_all(whole, "row", split_axis=1, concat_axis=0, tiled=True)
        solved = lax.psum_scatter(
            sum_terms(moved, inv_upper[section]).astype(jnp.bfloat16),
            "row",
            scatter_dimension=0,
            tiled=True,
        ).astype(jnp.float32)
        solutions[section] = solved
        if section > 0:
            pair_index = np.array(
                [section * (section - 1) // 2 + tile for tile in range(section)], dtype=np.int32
            )
            projections = jnp.einsum(
                "nw,mwr->mnr",
                solved.astype(jnp.bfloat16),
                up_right[pair_index],
                preferred_element_type=jnp.float32,
            )
            leading = lax.psum(projections[-1:].astype(jnp.bfloat16), "col").astype(jnp.float32)
            if section > 1:
                remaining = lax.psum(projections[:-1].astype(jnp.bfloat16), "col").astype(
                    jnp.float32
                )
                summed = jnp.concatenate([remaining, leading], axis=0)
            else:
                summed = leading
            masked = (summed * rank_mask(up_ranks, pair_index, rank_cols)[:, None, :]).astype(
                jnp.bfloat16
            )
            update = jnp.einsum(
                "mnr,mwr->mnw", masked, up_left[pair_index], preferred_element_type=jnp.float32
            )
            state = state.at[:section].add(-update)
    return jnp.stack(solutions)


MESH = pl.DeviceIdType.MESH
STREAMS = 8
LAG = {"start": 0, "cross": 1.1, "spread": 3.1, "multiply": 4.6, "share": 6.3, "relay1": 7.3, "relay2": 9.1, "finish": 10.4, "late": 14.3}
LAST = {"relay1": 6.6, "relay2": 7.8, "finish": 8.9}
TURN = 1.0


def schedule(streams, tiles):
    order = []
    for back in range(2):
        for stream in range(streams):
            spans = [(stage, lag, 0, tiles - (stage in LAST)) for stage, lag in LAG.items()]
            spans += [(stage, lag, tiles - 1, tiles) for stage, lag in LAST.items()]
            for stage, lag, first, end in spans:
                at = (lag + stream + back * TURN) / streams
                order.append(
                    (at - int(at), int(at), back * tiles + first, back * tiles + end, stream, stage)
                )
    return sorted(order, key=lambda event: (event[0], -event[1]))


def kernel(
    shape, rhs, low_left, low_right, up_left, up_right, masks, inv_lower, inv_upper, out,
    inv, left, right, source, crossing, moved, own, chunks, arrived, near, near_in, proj, proj_in, far, far_in,
    rhs_sem, load_sem, factor_sem, w_send, w_recv, g0_send, g0_recv, g1_send, g1_recv, g2_send, g2_recv, r_send, r_recv,
    n_send, n_recv, p_send, p_recv, f_send, f_recv,
):
    tiles, rows, cols, chips, streams, part = shape
    pairs = low_left.shape[0]
    wide = out.shape[2]
    lanes = inv_lower.shape[2]
    piece = wide // cols
    row, col = lax.axis_index("row"), lax.axis_index("col")
    chip, core = lax.div(row, 2), lax.rem(row, 2)
    steps = 2 * tiles

    def remote(src, dst, send, recv, to_row, to_col):
        return pltpu.make_async_remote_copy(
            src_ref=src, dst_ref=dst, send_sem=send, recv_sem=recv,
            device_id=(to_row, to_col), device_id_type=MESH,
        )

    def inverse_of(step):
        return inv_lower.at[step] if step < tiles else inv_upper.at[steps - 1 - step]

    def half(step, which):
        return inv.at[step, :, pl.ds(pl.multiple_of(which * lanes, lanes), lanes)]

    def load_inverse(step):
        return pltpu.make_async_copy(inverse_of(step), half(step, core), load_sem.at[step])

    def lend_inverse(step):
        return remote(
            inverse_of(step), half(step, core), w_send.at[step], w_recv.at[step], row + 1 - 2 * core, col
        )

    factors = [
        (low_right, right.at[pl.ds(0, pairs)]), (low_left, left.at[pl.ds(0, pairs)]),
        (up_right, right.at[pl.ds(pairs, pairs)]), (up_left, left.at[pl.ds(pairs, pairs)]),
    ]
    factors = [pltpu.make_async_copy(a, b, factor_sem.at[k]) for k, (a, b) in enumerate(factors)]
    sides = [pltpu.make_async_copy(rhs.at[k], out.at[k], rhs_sem.at[k]) for k in range(tiles)]
    sides[0].start()
    for step in range(steps):
        lend_inverse(step).start()
        load_inverse(step).start()
        if step < tiles:
            factors[step].start()
            if step + 1 < tiles:
                sides[step + 1].start()
    far[...] = jnp.zeros_like(far)
    sides[0].wait()

    def own_lanes():
        return pl.ds(pl.multiple_of(col * piece, piece), piece)

    def geometry(step):
        back = lax.div(step, tiles)
        section = step + back * (2 * tiles - 1 - 2 * step)
        count = (1 - back) * (tiles - 1 - section) + back * section
        return back, section, count

    def tile_of(back, section, v):
        tile = section + (1 - 2 * back) * (1 + v)
        high = back * section + (1 - back) * tile
        low = section + tile - high
        return tile, back * pairs + lax.div(high * (high - 1), 2) + low

    def place(stream):
        return pl.ds(stream * part, part)

    def side_of(step):
        return lax.rem(step, 2)

    def g0(step, stream, hop):
        to = lax.rem(col + hop, cols)
        return remote(
            source.at[stream, :, pl.ds(pl.multiple_of(to * piece, piece), piece)],
            crossing.at[side_of(step), stream, col],
            g0_send.at[stream, hop], g0_recv.at[stream, side_of(step), col],
            row, to,
        )

    def g1(step, stream, hop):
        to = lax.rem(chip + hop, chips)
        return remote(
            crossing.at[side_of(step), stream, to],
            moved.at[side_of(step), stream, chip, :, own_lanes()],
            g1_send.at[stream, hop], g1_recv.at[stream, side_of(step), chip],
            2 * to + core, col,
        )

    def g2(step, stream, hop):
        view = moved.at[side_of(step), stream, :, :, own_lanes()]
        return remote(
            view, view, g2_send.at[stream, hop], g2_recv.at[stream, side_of(step), hop],
            row, lax.rem(col + hop, cols),
        )

    def pass_on(step, stream, owner, way):
        side = side_of(step)
        to = chip + way
        slot = owner + lax.div(1 - way, 2) * jnp.where(owner == to, chips - owner, 0)
        return remote(
            chunks.at[side, stream, owner], arrived.at[side, stream, slot],
            r_send.at[stream, side, owner], r_recv.at[stream, side, slot],
            2 * to + core, col,
        )

    def took(step, stream, slot):
        side = side_of(step)
        view = arrived.at[side, stream, slot]
        pltpu.make_async_copy(view, view, r_recv.at[stream, side, slot]).wait()
        return arrived[side, stream, slot].astype(jnp.float32)

    def line(step, stream, leg):
        side = side_of(step)
        up, down = chip == leg, chip == chips - 1 - leg

        @pl.when(jnp.logical_or(up, down))
        def _():
            way = jnp.where(up, 1, -1)

            def one(k, carry):
                owner = jnp.where(up, chips - 1 - k, k)
                total = own[side, stream, owner]
                if leg > 0:
                    total += took(step, stream, owner)
                chunks[side, stream, owner] = total.astype(jnp.bfloat16)
                pass_on(step, stream, owner, way).start()
                return carry

            lax.fori_loop(0, chips - 1 - leg, one, 0)

    def near_copy(step, stream, hop):
        to = lax.rem(chip + hop, chips)
        return remote(
            near.at[stream, to], near_in.at[side_of(step), stream, hop],
            n_send.at[stream, hop], n_recv.at[stream, side_of(step), hop],
            2 * to + core, col,
        )

    def project(step, stream, hop):
        return remote(
            proj.at[stream], proj_in.at[side_of(step), stream, hop],
            p_send.at[stream, hop], p_recv.at[stream, side_of(step), hop],
            row, lax.rem(col + hop, cols),
        )

    def project_far(step, stream, hop):
        return remote(
            far.at[stream], far_in.at[side_of(step), stream, hop],
            f_send.at[stream, hop], f_recv.at[stream, side_of(step), hop],
            row, lax.rem(col + hop, cols),
        )

    def subtract(tile, pair, stream, total):
        masked = (total * masks[pair]).astype(jnp.bfloat16)
        out[tile, place(stream), :] -= times_inverse(masked, left[pair])

    def start(step, stream):
        @pl.when(jnp.logical_and(step > 0, step != tiles))
        def _():
            if stream == 0:

                @pl.when(step == 1)
                def _():
                    for k in range(1, tiles):
                        sides[k].wait()
                    for k in range(1, 4):
                        factors[k].wait()

            back, section, _ = geometry(step - 1)
            tile, pair = tile_of(back, section, 0)
            for hop in range(1, cols):
                project(step - 1, stream, hop).wait()
            total = proj[stream].astype(jnp.float32)
            for hop in range(1, cols):
                total += proj_in[side_of(step - 1), stream, hop].astype(jnp.float32)
            subtract(tile, pair, stream, total)

        _, section, _ = geometry(step)
        source[stream] = out[section, place(stream), :].astype(jnp.bfloat16)
        for hop in range(1, cols):
            g0(step, stream, hop).start()
        pltpu.make_async_copy(
            source.at[stream, :, own_lanes()], crossing.at[side_of(step), stream, col],
            g0_recv.at[stream, side_of(step), col],
        ).start()

    def cross(step, stream):
        side = side_of(step)
        for k in range(cols):
            view = crossing.at[side, stream, k]
            pltpu.make_async_copy(view, view, g0_recv.at[stream, side, k]).wait()
        for hop in range(1, chips):
            g1(step, stream, hop).start()
        pltpu.make_async_copy(
            crossing.at[side, stream, chip], moved.at[side, stream, chip, :, own_lanes()],
            g1_recv.at[stream, side, chip],
        ).start()
        for hop in range(1, cols):
            g0(step, stream, hop).wait_send()

    def spread(step, stream):
        for k in range(chips):
            view = moved.at[side_of(step), stream, k, :, own_lanes()]
            pltpu.make_async_copy(view, view, g1_recv.at[stream, side_of(step), k]).wait()
        for hop in range(1, cols):
            g2(step, stream, hop).start()
        for hop in range(1, chips):
            g1(step, stream, hop).wait_send()

    def multiply(step, stream):
        side = side_of(step)
        back, section, count = geometry(step)
        if stream == 0:
            view = half(step, core)
            pltpu.make_async_copy(view, view, load_sem.at[step]).wait()
            view = half(step, 1 - core)
            pltpu.make_async_copy(view, view, w_recv.at[step]).wait()

            @pl.when(step == 0)
            def _():
                factors[0].wait()

        for hop in range(1, cols):
            view = moved.at[
                side, stream, :, :,
                pl.ds(pl.multiple_of(lax.rem(col + cols - hop, cols) * piece, piece), piece),
            ]
            pltpu.make_async_copy(view, view, g2_recv.at[stream, side, hop]).wait()
        whole = moved[side, stream].reshape(chips * part, wide)
        terms = times_inverse(whole, inv[step])
        own[side, stream] = terms.reshape(chips, part, wide)

        @pl.when(count > 0)
        def _():
            _, pair = tile_of(back, section, 0)
            rounded = own[side, stream].reshape(chips * part, wide).astype(jnp.bfloat16)
            near[stream] = (
                jnp.dot(rounded, right[pair], preferred_element_type=jnp.float32)
                .astype(jnp.bfloat16)
                .reshape(chips, part, -1)
            )
            for hop in range(1, chips):
                near_copy(step, stream, hop).start()

        line(step, stream, 0)
        for hop in range(1, cols):
            g2(step, stream, hop).wait_send()

    def share(step, stream):
        _, _, count = geometry(step)

        @pl.when(count > 0)
        def _():
            for hop in range(1, chips):
                near_copy(step, stream, hop).wait()
            total = near[stream, chip].astype(jnp.float32)
            for hop in range(1, chips):
                total += near_in[side_of(step), stream, hop].astype(jnp.float32)
            proj[stream] = total.astype(jnp.bfloat16)
            for hop in range(1, cols):
                project(step, stream, hop).start()

    def finish(step, stream):
        side = side_of(step)
        back, section, count = geometry(step)
        out[section, place(stream), :] = own[side, stream, chip]

        @pl.when(chip > 0)
        def _():
            out[section, place(stream), :] += took(step, stream, chip)

        @pl.when(chip < chips - 1)
        def _():
            out[section, place(stream), :] += took(step, stream, chips)

        for owner in range(chips):

            @pl.when(chip != owner)
            def _():
                pass_on(step, stream, owner, jnp.where(owner > chip, 1, -1)).wait_send()

        @pl.when(count > 1)
        def _():
            rounded = out[section, place(stream), :].astype(jnp.bfloat16)

            def one(v, carry):
                _, pair = tile_of(back, section, v)
                far[stream, v - 1] = jnp.dot(
                    rounded, right[pair], preferred_element_type=jnp.float32
                ).astype(jnp.bfloat16)
                return carry

            lax.fori_loop(1, count, one, 0)
            for hop in range(1, cols):
                project_far(step, stream, hop).start()

    def late(step, stream):
        back, section, count = geometry(step)
        side = side_of(step)

        @pl.when(count > 1)
        def _():
            for hop in range(1, cols):
                project_far(step, stream, hop).wait()

            def one(v, carry):
                tile, pair = tile_of(back, section, v)
                total = far[stream, v - 1].astype(jnp.float32)
                for hop in range(1, cols):
                    total += far_in[side, stream, hop, v - 1].astype(jnp.float32)
                subtract(tile, pair, stream, total)
                return carry

            lax.fori_loop(1, count, one, 0)

    stages = {
        "start": start, "cross": cross, "spread": spread, "multiply": multiply, "share": share,
        "relay1": functools.partial(line, leg=1), "relay2": functools.partial(line, leg=2),
        "finish": finish, "late": late,
    }
    order = schedule(streams, tiles)
    latest = max(event[1] for event in order)

    def body(turn, carry):
        for _, shift, first, end, stream, stage in order:
            step = turn - shift

            @pl.when(jnp.logical_and(step >= first, step < end))
            def _():
                stages[stage](step, stream)

        return carry

    lax.fori_loop(0, steps + latest, body, 0)
    for step in range(steps):
        lend_inverse(step).wait_send()


def fused(
    rows, cols, streams, right_sides, low_left, low_right, up_left, up_right, low_ranks, up_ranks,
    inv_lower, inv_upper,
):
    tiles, held, wide = right_sides.shape
    pairs, _, rank_cols = low_left.shape
    chips = rows // 2
    part = held // streams
    masks = rank_mask(
        jnp.concatenate([low_ranks, up_ranks]), np.arange(2 * pairs), rank_cols
    ).reshape(2 * pairs, 1, rank_cols)
    half = jnp.bfloat16
    dma = pltpu.SemaphoreType.DMA
    later = max(tiles - 2, 1)
    scratch = [
        pltpu.VMEM((2 * tiles, wide, wide), half),
        pltpu.VMEM((2 * pairs, wide, rank_cols), half),
        pltpu.VMEM((2 * pairs, wide, rank_cols), half),
        pltpu.VMEM((streams, part, wide), half),
        pltpu.VMEM((2, streams, cols, part, wide // cols), half),
        pltpu.VMEM((2, streams, chips, part, wide), half),
        pltpu.VMEM((2, streams, chips, part, wide), jnp.float32),
        pltpu.VMEM((2, streams, chips, part, wide), half),
        pltpu.VMEM((2, streams, chips + 1, part, wide), half),
        pltpu.VMEM((streams, chips, part, rank_cols), half),
        pltpu.VMEM((2, streams, chips, part, rank_cols), half),
        pltpu.VMEM((streams, part, rank_cols), half),
        pltpu.VMEM((2, streams, cols, part, rank_cols), half),
        pltpu.VMEM((streams, later, part, rank_cols), half),
        pltpu.VMEM((2, streams, cols, later, part, rank_cols), half),
        dma((tiles,)), dma((2 * tiles,)), dma((4,)), dma((2 * tiles,)), dma((2 * tiles,)),
        dma((streams, cols)), dma((streams, 2, cols)),
        dma((streams, chips)), dma((streams, 2, chips)),
        dma((streams, cols)), dma((streams, 2, cols)),
        dma((streams, 2, chips)), dma((streams, 2, chips + 1)),
        dma((streams, chips)), dma((streams, 2, chips)),
        dma((streams, cols)), dma((streams, 2, cols)),
        dma((streams, cols)), dma((streams, 2, cols)),
    ]
    anywhere = pl.BlockSpec(memory_space=pl.ANY)
    vmem = pl.BlockSpec(memory_space=pltpu.VMEM)
    return pl.pallas_call(
        functools.partial(kernel, (tiles, rows, cols, chips, streams, part)),
        out_shape=jax.ShapeDtypeStruct(right_sides.shape, jnp.float32),
        in_specs=[anywhere] * 5 + [vmem] + [anywhere] * 2,
        out_specs=vmem,
        scratch_shapes=scratch,
        compiler_params=pltpu.CompilerParams(
            has_side_effects=True, vmem_limit_bytes=60 * 1024 * 1024
        ),
    )(right_sides, low_left, low_right, up_left, up_right, masks, inv_lower, inv_upper)


def pick(mesh):
    rows, cols = mesh.shape["row"], mesh.shape["col"]

    def run(right_sides, *rest):
        tiles, held, wide = right_sides.shape
        fits = rows == 8 and cols == 4 and tiles == 4 and wide == 2 * rest[-1].shape[2]
        if fits and wide % (128 * cols) == 0 and held % (16 * STREAMS) == 0:
            return fused(rows, cols, STREAMS, right_sides, *rest)
        return shards(right_sides, *rest)

    return run


def solution(mesh):
    in_specs = (
        P(None, "row", "col"),
        P(None, "col", None),
        P(None, "col", None),
        P(None, "col", None),
        P(None, "col", None),
        P(),
        P(),
        P(None, "col", "row"),
        P(None, "col", "row"),
    )
    out_specs = P(None, "row", "col")
    return jax.shard_map(pick(mesh), mesh=mesh, in_specs=in_specs, out_specs=out_specs, check_vma=False)
```
